32 devices in a mesh: row: 8 (over z, x), col: 4 (over y, core).
Axes of the slice: x: 2, y: 2, z: 4, core: 2. Of those that a mesh axis runs over, the one named last changes fastest.
Arguments:
- hidden: bfloat16 [4, 20480, 768], P(None, ('row', 'col')), may hold values from -6 to 6
- grad_out: bfloat16 [4, 20480, 1024], P(None, ('row', 'col')), may hold values from -6 to 6
- counts: int32 [32, 4], P(('row', 'col')), may hold values from 1 to 640, as said below
- shadow_ids: int32 [4], replicated, may hold values from 0 to 59, as said below
- master: float32 [60, 768, 1024], P(None, 'row', 'col'), may hold values from -0.21875 to 0.21875
- momentum: float32 [60, 768, 1024], P(None, 'row', 'col'), may hold values from -6 to 6
Outputs:
- master_out: float32 [60, 768, 1024], P(None, 'row', 'col')
- momentum_out: float32 [60, 768, 1024], P(None, 'row', 'col')
- shadow_out: bfloat16 [4, 768, 1024], P(None, 'row')
The draws below stay inside these ranges and needn't reach their ends.
Inputs may be any that keep to these rules, and one draw needn't show every extreme that they name: counts are at most 640, and some device reaches 640 for some shadowed expert. `shadow_ids`: the 4 ids are distinct, and experts 0 and 59 are always among them.
All inputs are finite; a program needn't handle non-finite values.
Results may differ from the reference program's by a relative error of at most 0.007.
Values may be sent and summed in bfloat16 or wider, within the bound.
No kernel may reach another device: no remote copies, remote signals or barrier semaphores. Data moves between devices by JAX's collectives and lax.ppermute only.
A program may use at most 128 MiB of HBM per device.

```python
import jax
import jax.numpy as jnp
from jax import lax

D_WIN = 1024
F_WIN = 768
EXPERTS = 60
SHADOW = 4
CAP = 640
TOKENS = 20480
N_ROW = 8
N_COL = 4


def draw_counts(key, part):
    devices = N_ROW * N_COL
    first = jax.random.randint(jax.random.fold_in(key, 11), (devices, SHADOW), 1, CAP + 1)
    second = jax.random.randint(jax.random.fold_in(key, 12), (devices, SHADOW), 1, CAP + 1)
    values = jnp.minimum(first, second)
    chosen = jax.random.randint(jax.random.fold_in(key, 13), (), 0, devices * SHADOW)
    flat_index = jnp.arange(devices * SHADOW, dtype=jnp.int32).reshape(devices, SHADOW)
    return jnp.where(flat_index == chosen, CAP, values).astype(jnp.int32)


def draw_shadow_ids(key, part):
    middle = jax.random.permutation(jax.random.fold_in(key, 21), EXPERTS - 2) + 1
    ends = jnp.array([0, EXPERTS - 1], dtype=jnp.int32)
    chosen = jnp.concatenate([ends, middle[:SHADOW - 2].astype(jnp.int32)])
    return jax.random.permutation(jax.random.fold_in(key, 22), chosen).astype(jnp.int32)


def raised(values, rng, source, target, shards_of, factor):
    owner, partner = [(jnp.arange(values.shape[dim]) // (values.shape[dim] // shards_of)).reshape([-1 if axis == dim else 1 for axis in range(values.ndim)]) for dim in (source, target)]
    chosen = jax.random.permutation(rng, shards_of)[partner]
    strong = (owner == chosen) | (owner == (partner + shards_of // 2) % shards_of)
    return jnp.where(strong, factor * values, values)


def levels(rng, dims, pieces, smallest, high):
    level, own = 1.0, jax.random.fold_in(rng, 6)
    for axis_at, blocks in pieces:
        draws = jnp.exp(jax.random.uniform(jax.random.fold_in(own, axis_at), (blocks,), jnp.float32, smallest / len(pieces), high / len(pieces)))
        level = level * jnp.repeat(draws, dims[axis_at] // blocks).reshape([-1 if axis == axis_at else 1 for axis in range(len(dims))])
    return level


def gaussian(key, dims, spread, limit, cuts=(), kind=jnp.bfloat16):
    gain = levels(key, dims, cuts, -0.22, 0.18) if cuts else 1.0
    drawn = jax.random.normal(key, dims, jnp.float32) * spread * gain
    return jnp.minimum(jnp.maximum(drawn, -limit), limit).astype(kind)


def gaussian_with(stream_key, dims, width, most, cuts, heavy, kind=jnp.bfloat16):
    values = width * jax.random.normal(stream_key, dims, jnp.float32)
    if cuts:
        values = values * levels(stream_key, dims, cuts, -0.22, 0.18)
    return jnp.clip(raised(values, jax.random.fold_in(stream_key, 3), *heavy), -most, most).astype(kind)


def setup_inputs(seed: int = 0) -> dict:
    key_list = jax.random.split(jax.random.key(seed), 7)
    hidden = gaussian(key_list[0], (SHADOW, TOKENS, F_WIN), 1.0, 6.0, ((1, 32),))
    grad_out = gaussian_with(key_list[1], (SHADOW, TOKENS, D_WIN), 1.0, 6.0, ((1, 32),), (1, 2, 32, 2.75))
    counts = draw_counts(jax.random.fold_in(key_list[6], 71), 0)
    shadow_ids = draw_shadow_ids(jax.random.fold_in(key_list[6], 71), 0)
    master = gaussian(key_list[4], (EXPERTS, F_WIN, D_WIN), F_WIN ** -0.5, 0.21875, ((1, 8), (2, 4)), jnp.float32)
    momentum = gaussian(key_list[5], (EXPERTS, F_WIN, D_WIN), 1.0, 6.0, ((1, 8), (2, 4)), jnp.float32)
    return dict(hidden=hidden, grad_out=grad_out, counts=counts, shadow_ids=shadow_ids, master=master, momentum=momentum)


def reference(hidden, grad_out, counts, shadow_ids, master, momentum):
    devices = N_ROW * N_COL
    positions = jnp.arange(CAP, dtype=jnp.int32)

    def one_expert(expert):
        live_mask = (positions[None, :] < counts[:, expert][:, None]).reshape(-1)
        masked = jnp.where(live_mask[:, None], hidden[expert], jnp.zeros((), jnp.bfloat16))
        return jnp.dot(masked.T, grad_out[expert], preferred_element_type=jnp.float32)

    gradient = lax.map(one_expert, jnp.arange(SHADOW, dtype=jnp.int32))
    gradient = gradient * jnp.float32((CAP * devices) ** -0.5)
    new_momentum = 0.9 * momentum[shadow_ids] + gradient
    new_master = master[shadow_ids] - 0.01 * new_momentum
    momentum_out = momentum.at[shadow_ids].set(new_momentum)
    master_out = master.at[shadow_ids].set(new_master)
    return master_out, momentum_out, new_master.astype(jnp.bfloat16)
```

```python
import jax
import jax.numpy as jnp
from jax import lax
from jax.experimental import pallas as pl
from jax.experimental.pallas import tpu as pltpu
from jax.sharding import PartitionSpec as P

momentum_decay = 0.9
step_size = 0.01


def bits_of(size):
    return size.bit_length() - 1


def chunk_count(rows):
    return 3 if rows % 48 == 0 else 1


def half_gradient(hidden, grad_out, live_counts, core, rows, cols, chunks):
    experts, tokens, features = hidden.shape
    outs = grad_out.shape[2]
    block_f, block_d = features // rows, outs // cols
    piece = block_f // chunks
    halves = cols // 2

    if block_d % 128:
        live = jnp.arange(tokens, dtype=jnp.int32)[None, :] < live_counts[:, None]
        masked = jnp.where(live[:, :, None], hidden, jnp.zeros((), hidden.dtype))
        part = lax.dynamic_index_in_dim(
            grad_out.reshape(experts, tokens, halves, 2, block_d), core, 3, keepdims=False
        )
        full = jnp.einsum("etf,etcd->cfed", masked, part, preferred_element_type=jnp.float32)
        full = full.astype(jnp.bfloat16).reshape(halves, rows, chunks, piece, experts, block_d)
        full = full.transpose(2, 0, 1, 4, 3, 5)
        return [full[j] for j in range(chunks)]

    def body(core_ref, counts_ref, h_ref, *refs):
        g_refs, o_refs = refs[:halves], refs[halves:]
        e = pl.program_id(0)
        live = lax.broadcasted_iota(jnp.int32, (tokens, 1), 0) < counts_ref[e]
        h = jnp.where(live, h_ref[0], jnp.zeros((), h_ref.dtype))
        for y in range(halves):
            res = lax.dot_general(
                h, g_refs[y][0], (((0,), (0,)), ((), ())), preferred_element_type=jnp.float32
            )
            res = res.astype(jnp.bfloat16).reshape(rows, chunks, piece, block_d)
            for j in range(chunks):
                o_refs[j][y, :, 0] = res[:, j]

    def g_map(y):
        return lambda e, core_ref, counts_ref: (e, 0, 2 * y + core_ref[0])

    out = jax.ShapeDtypeStruct((halves, rows, experts, piece, block_d), jnp.bfloat16)
    return pl.pallas_call(
        body,
        grid_spec=pltpu.PrefetchScalarGridSpec(
            num_scalar_prefetch=2,
            grid=(experts,),
            in_specs=[pl.BlockSpec((1, tokens, features), lambda e, a, b: (e, 0, 0))]
            + [pl.BlockSpec((1, tokens, block_d), g_map(y)) for y in range(halves)],
            out_specs=[
                pl.BlockSpec((halves, rows, 1, piece, block_d), lambda e, a, b: (0, 0, e, 0, 0))
                for _ in range(chunks)
            ],
        ),
        out_shape=[out] * chunks,
        cost_estimate=pl.CostEstimate(
            flops=experts * tokens * features * outs, bytes_accessed=8000000, transcendentals=0
        ),
    )(core.reshape(1), live_counts, hidden, *([grad_out] * halves))


def update(shadow_ids, master, momentum, pairs, scale):
    experts = shadow_ids.shape[0]
    block_f, block_d = master.shape[1:]
    chunks = len(pairs)
    piece = block_f // chunks

    def body(ids_ref, *refs):
        sums = refs[: 2 * chunks]
        w_ref, m_ref, w_out, m_out, s_out = refs[2 * chunks :]
        for j in range(chunks):
            at = pl.ds(j * piece, piece)
            total = sums[2 * j][0].astype(jnp.float32) + sums[2 * j + 1][0].astype(jnp.float32)
            new_m = momentum_decay * m_ref[0, at] + total * scale
            new_w = w_ref[0, at] - step_size * new_m
            m_out[0, at] = new_m
            w_out[0, at] = new_w
            s_out[0, at] = new_w.astype(jnp.bfloat16)

    row = pl.BlockSpec((1, block_f, block_d), lambda e, ids: (ids[e], 0, 0))
    part = pl.BlockSpec((1, piece, block_d), lambda e, ids: (e, 0, 0))
    return pl.pallas_call(
        body,
        grid_spec=pltpu.PrefetchScalarGridSpec(
            num_scalar_prefetch=1,
            grid=(experts,),
            in_specs=[part] * (2 * chunks) + [row, row],
            out_specs=[row, row, pl.BlockSpec((1, block_f, block_d), lambda e, ids: (e, 0, 0))],
        ),
        out_shape=[
            jax.ShapeDtypeStruct(master.shape, master.dtype),
            jax.ShapeDtypeStruct(momentum.shape, momentum.dtype),
            jax.ShapeDtypeStruct((experts, block_f, block_d), jnp.bfloat16),
        ],
        input_output_aliases={1 + 2 * chunks: 0, 2 + 2 * chunks: 1},
    )(shadow_ids, *[a for pair in pairs for a in pair], master, momentum)


def swap(values, name, bit):
    size = lax.axis_size(name)
    return lax.ppermute(values, name, [(i, i ^ (1 << bit)) for i in range(size)])


def pick(values, axis, index):
    return lax.dynamic_index_in_dim(values, index, axis, keepdims=False)


def add(a, b):
    return (a.astype(jnp.float32) + b.astype(jnp.float32)).astype(jnp.bfloat16)


def shards(hidden, grad_out, counts, shadow_ids, master, momentum):
    rows, cols = lax.axis_size("row"), lax.axis_size("col")
    place = {"row": lax.axis_index("row"), "col": lax.axis_index("col")}
    experts = hidden.shape[0]
    block_f, block_d = master.shape[1:]
    chunks = chunk_count(block_f)
    live_counts = counts[0]
    core = place["col"] & 1
    away = half_gradient(hidden, grad_out, live_counts, 1 - core, rows, cols, chunks)
    came = [swap(a, "col", 0) for a in away]
    own = half_gradient(hidden, grad_out, live_counts, core, rows, cols, chunks)

    col_bits = [("col", k) for k in range(1, bits_of(cols))]
    row_bits = [("row", k) for k in range(bits_of(rows))]
    layout = col_bits[::-1] + row_bits[::-1]
    early = col_bits[:1] + row_bits[:2]
    late = col_bits[1:] + row_bits[2:]
    state = []
    for j in range(chunks):
        shape = (2,) * len(layout) + own[j].shape[2:]
        turn = j % len(early)
        order = early[turn:] + early[:turn] + late
        state.append([own[j].reshape(shape), came[j].reshape(shape), list(layout), order])
    for step in range(len(layout)):
        for entry in state:
            mine, got, left, order = entry
            name, bit = order[step]
            axis = left.index((name, bit))
            left.remove((name, bit))
            here = (place[name] >> bit) & 1
            send = add(pick(mine, axis, 1 - here), pick(got, axis, 1 - here))
            entry[1] = swap(send, name, bit)
            entry[0] = add(pick(mine, axis, here), pick(got, axis, here))
    pairs = [(entry[0], entry[1]) for entry in state]

    devices = rows * cols
    scale = float((hidden.shape[1] * devices) ** (-0.5))
    master_out, momentum_out, shadow = update(shadow_ids, master, momentum, pairs, scale)
    shadow_out = lax.all_gather(shadow, "col", axis=2, tiled=True)
    return (master_out, momentum_out, shadow_out)


def solution(mesh):
    return jax.shard_map(
        shards,
        mesh=mesh,
        in_specs=(
            P(None, ("row", "col"), None),
            P(None, ("row", "col"), None),
            P(("row", "col"), None),
            P(),
            P(None, "row", "col"),
            P(None, "row", "col"),
        ),
        out_specs=(P(None, "row", "col"), P(None, "row", "col"), P(None, "row", None)),
        check_vma=False,
    )
```

```python
import jax
import jax.numpy as jnp
from jax import lax
from jax.experimental import pallas as pl
from jax.experimental.pallas import tpu as pltpu
from jax.sharding import PartitionSpec as P

momentum_decay = 0.9
step_size = 0.01


def bits_of(size):
    return size.bit_length() - 1


def chunk_count(rows):
    return 3 if rows % 48 == 0 else 1


def flat_index(order, place):
    total = 0
    for name, bit in order:
        total = total * 2 + ((place[name] >> bit) & 1)
    return total


def half_gradient(hidden, grad_out, live_counts, core, place, rows, cols, orders):
    experts, tokens, features = hidden.shape
    outs = grad_out.shape[2]
    chunks = len(orders)
    block_f, block_d = features // rows, outs // cols
    piece = block_f // chunks
    halves = cols // 2
    blocks = halves * rows

    if block_d % 128:
        live = jnp.arange(tokens, dtype=jnp.int32)[None, :] < live_counts[:, None]
        masked = jnp.where(live[:, :, None], hidden, jnp.zeros((), hidden.dtype))
        part = lax.dynamic_index_in_dim(
            grad_out.reshape(experts, tokens, halves, 2, block_d), core, 3, keepdims=False
        )
        full = jnp.einsum("etf,etcd->cfed", masked, part, preferred_element_type=jnp.float32)
        full = full.astype(jnp.bfloat16).reshape(halves, rows, chunks, piece, experts, block_d)
        full = full.transpose(2, 0, 1, 4, 3, 5)
        plain = [("col", k) for k in range(bits_of(cols) - 1, 0, -1)]
        plain += [("row", k) for k in range(bits_of(rows) - 1, -1, -1)]
        given = []
        for j, order in enumerate(orders):
            split = full[j].reshape((2,) * len(plain) + full.shape[3:])
            perm = [plain.index(at) for at in order]
            split = split.transpose(perm + list(range(len(plain), split.ndim)))
            split = split.reshape((blocks,) + full.shape[3:])
            given.append(jnp.take(split, jnp.arange(blocks) ^ flat_index(order, place), axis=0))
        return given

    def body(where_ref, counts_ref, h_ref, *refs):
        g_refs, o_refs = refs[:halves], refs[halves:]
        e = pl.program_id(0)
        row = where_ref[1]
        live = lax.broadcasted_iota(jnp.int32, (tokens, 1), 0) < counts_ref[e]
        h = jnp.where(live, h_ref[0], jnp.zeros((), h_ref.dtype))
        for y in range(halves):
            res = lax.dot_general(
                h, g_refs[y][0], (((0,), (0,)), ((), ())), preferred_element_type=jnp.float32
            )
            res = res.astype(jnp.bfloat16).reshape(rows, chunks, piece, block_d)
            for r in range(rows):
                spot = {"col": 2 * y, "row": r ^ row}
                for j in range(chunks):
                    o_refs[j][flat_index(orders[j], spot), 0] = res[r, j]

    def g_map(y):
        return lambda e, where_ref, counts_ref: (e, 0, ((2 * y) ^ where_ref[2]) + where_ref[0])

    where = jnp.stack([core, place["row"], place["col"] - (place["col"] & 1)]).astype(jnp.int32)
    out = jax.ShapeDtypeStruct((blocks, experts, piece, block_d), jnp.bfloat16)
    return pl.pallas_call(
        body,
        grid_spec=pltpu.PrefetchScalarGridSpec(
            num_scalar_prefetch=2,
            grid=(experts,),
            in_specs=[pl.BlockSpec((1, tokens, features), lambda e, a, b: (e, 0, 0))]
            + [pl.BlockSpec((1, tokens, block_d), g_map(y)) for y in range(halves)],
            out_specs=[
                pl.BlockSpec((blocks, 1, piece, block_d), lambda e, a, b: (0, e, 0, 0))
                for _ in range(chunks)
            ],
        ),
        out_shape=[out] * chunks,
        cost_estimate=pl.CostEstimate(
            flops=experts * tokens * features * outs, bytes_accessed=8000000, transcendentals=0
        ),
    )(where, live_counts, hidden, *([grad_out] * halves))


def copies(token, master, momentum):
    experts, block_f, block_d = master.shape
    step = max(n for n in range(1, 7) if experts % n == 0)

    def body(token_ref, w_ref, m_ref, w_out, m_out):
        w_out[...] = w_ref[...]
        m_out[...] = m_ref[...]

    block = pl.BlockSpec((step, block_f, block_d), lambda i: (i, 0, 0))
    return pl.pallas_call(
        body,
        grid=(experts // step,),
        in_specs=[pl.BlockSpec(memory_space=pl.ANY), block, block],
        out_specs=[block, block],
        out_shape=[
            jax.ShapeDtypeStruct(master.shape, master.dtype),
            jax.ShapeDtypeStruct(momentum.shape, momentum.dtype),
        ],
        cost_estimate=pl.CostEstimate(
            flops=2 * 10**9, bytes_accessed=16 * master.size, transcendentals=0
        ),
    )(token, master, momentum)


def shadow_rows(token, shadow_ids, master, momentum):
    experts = shadow_ids.shape[0]
    block_f, block_d = master.shape[1:]

    def body(ids_ref, token_ref, w_ref, m_ref, w_out, m_out):
        w_out[...] = w_ref[...]
        m_out[...] = m_ref[...]

    row = pl.BlockSpec((1, block_f, block_d), lambda e, ids: (ids[e], 0, 0))
    own = pl.BlockSpec((1, block_f, block_d), lambda e, ids: (e, 0, 0))
    out = jax.ShapeDtypeStruct((experts, block_f, block_d), jnp.float32)
    return pl.pallas_call(
        body,
        grid_spec=pltpu.PrefetchScalarGridSpec(
            num_scalar_prefetch=1,
            grid=(experts,),
            in_specs=[pl.BlockSpec(memory_space=pl.ANY), row, row],
            out_specs=[own, own],
        ),
        out_shape=[out, out],
        cost_estimate=pl.CostEstimate(
            flops=5 * 10**8, bytes_accessed=16 * experts * block_f * block_d, transcendentals=0
        ),
    )(shadow_ids, token, master, momentum)


def place_rows(shadow_ids, new_master, new_momentum, master, momentum):
    experts, block_f, block_d = new_master.shape

    def body(ids_ref, nw_ref, nm_ref, w_ref, m_ref, w_out, m_out):
        w_out[...] = nw_ref[...]
        m_out[...] = nm_ref[...]

    row = pl.BlockSpec((1, block_f, block_d), lambda e, ids: (ids[e], 0, 0))
    own = pl.BlockSpec((1, block_f, block_d), lambda e, ids: (e, 0, 0))
    whole = pl.BlockSpec(memory_space=pl.ANY)
    return pl.pallas_call(
        body,
        grid_spec=pltpu.PrefetchScalarGridSpec(
            num_scalar_prefetch=1,
            grid=(experts,),
            in_specs=[own, own, whole, whole],
            out_specs=[row, row],
        ),
        out_shape=[
            jax.ShapeDtypeStruct(master.shape, master.dtype),
            jax.ShapeDtypeStruct(momentum.shape, momentum.dtype),
        ],
        input_output_aliases={3: 0, 4: 1},
        cost_estimate=pl.CostEstimate(
            flops=5 * 10**8, bytes_accessed=16 * experts * block_f * block_d, transcendentals=0
        ),
    )(shadow_ids, new_master, new_momentum, master, momentum)


def swap(values, name, bit):
    size = lax.axis_size(name)
    return lax.ppermute(values, name, [(i, i ^ (1 << bit)) for i in range(size)])


def add(a, b):
    return (a.astype(jnp.float32) + b.astype(jnp.float32)).astype(jnp.bfloat16)


def shards(hidden, grad_out, counts, shadow_ids, master, momentum):
    rows, cols = lax.axis_size("row"), lax.axis_size("col")
    place = {"row": lax.axis_index("row"), "col": lax.axis_index("col")}
    block_f, block_d = master.shape[1:]
    chunks = chunk_count(block_f)
    live_counts = counts[0]
    core = place["col"] & 1

    col_bits = [("col", k) for k in range(1, bits_of(cols))]
    row_bits = [("row", k) for k in range(bits_of(rows))]
    early = col_bits[:1] + row_bits[:2]
    late = col_bits[1:] + row_bits[2:]
    turns = [j % len(early) for j in range(chunks)]
    orders = [early[t:] + early[:t] + late for t in turns]

    away = half_gradient(hidden, grad_out, live_counts, 1 - core, place, rows, cols, orders)
    got = [swap(a, "col", 0) for a in away]
    own = list(half_gradient(hidden, grad_out, live_counts, core, place, rows, cols, orders))

    for step in range(len(early)):
        sends = []
        for j in range(chunks):
            half = own[j].shape[0] // 2
            sends.append(add(own[j][half:], got[j][half:]))
            own[j], came = add(own[j][:half], got[j][:half]), sends[j]
            got[j] = swap(came, *orders[j][step])
        if step == 0:
            token = sum(s[0, 0, :8] for s in sends)
            made = copies(token, master, momentum) + shadow_rows(token, shadow_ids, master, momentum)
            made, own = lax.optimization_barrier((made, own))
    own = jnp.concatenate(own, axis=2)
    got = jnp.concatenate(got, axis=2)
    for at in late:
        half = own.shape[0] // 2
        send = add(own[half:], got[half:])
        own, got = add(own[:half], got[:half]), swap(send, *at)
    total = own[0].astype(jnp.float32) + got[0].astype(jnp.float32)

    master_copy, momentum_copy, old_master, old_momentum = made
    devices = rows * cols
    scale = jnp.float32((hidden.shape[1] * devices) ** (-0.5))
    new_momentum = momentum_decay * old_momentum + total * scale
    new_master = old_master - step_size * new_momentum
    shadow = new_master.astype(jnp.bfloat16)[None]
    for bit in range(bits_of(cols) - 1, -1, -1):
        other = swap(shadow, "col", bit)
        shadow = jnp.stack([shadow, other], axis=1).reshape((-1,) + shadow.shape[1:])
    master_out, momentum_out = place_rows(
        shadow_ids, new_master, new_momentum, master_copy, momentum_copy
    )
    shadow_out = jnp.concatenate(
        [lax.dynamic_index_in_dim(shadow, c ^ place["col"], 0, keepdims=False) for c in range(cols)],
        axis=2,
    )
    return (master_out, momentum_out, shadow_out)


def solution(mesh):
    return jax.shard_map(
        shards,
        mesh=mesh,
        in_specs=(
            P(None, ("row", "col"), None),
            P(None, ("row", "col"), None),
            P(("row", "col"), None),
            P(),
            P(None, "row", "col"),
            P(None, "row", "col"),
        ),
        out_specs=(P(None, "row", "col"), P(None, "row", "col"), P(None, "row", None)),
        check_vma=False,
    )
```

```python
import jax
import jax.numpy as jnp
from jax import lax
from jax.experimental import pallas as pl
from jax.experimental.pallas import tpu as pltpu
from jax.sharding import PartitionSpec as P

momentum_decay = 0.9
step_size = 0.01


def bits_of(size):
    return size.bit_length() - 1


def chunk_count(rows):
    return 3 if rows % 48 == 0 else 1


def flat_index(order, place):
    total = 0
    for name, bit in order:
        total = total * 2 + ((place[name] >> bit) & 1)
    return total


def half_gradient(hidden, grad_out, live_counts, core, place, rows, cols, orders):
    experts, tokens, features = hidden.shape
    outs = grad_out.shape[2]
    chunks = len(orders)
    block_f, block_d = features // rows, outs // cols
    piece = block_f // chunks
    halves = cols // 2
    blocks = halves * rows

    if block_d % 128:
        live = jnp.arange(tokens, dtype=jnp.int32)[None, :] < live_counts[:, None]
        masked = jnp.where(live[:, :, None], hidden, jnp.zeros((), hidden.dtype))
        part = lax.dynamic_index_in_dim(
            grad_out.reshape(experts, tokens, halves, 2, block_d), core, 3, keepdims=False
        )
        full = jnp.einsum("etf,etcd->cfed", masked, part, preferred_element_type=jnp.float32)
        full = full.astype(jnp.bfloat16).reshape(halves, rows, chunks, piece, experts, block_d)
        full = full.transpose(2, 0, 1, 4, 3, 5)
        plain = [("col", k) for k in range(bits_of(cols) - 1, 0, -1)]
        plain += [("row", k) for k in range(bits_of(rows) - 1, -1, -1)]
        given = []
        for j, order in enumerate(orders):
            split = full[j].reshape((2,) * len(plain) + full.shape[3:])
            perm = [plain.index(at) for at in order]
            split = split.transpose(perm + list(range(len(plain), split.ndim)))
            split = split.reshape((blocks,) + full.shape[3:])
            given.append(jnp.take(split, jnp.arange(blocks) ^ flat_index(order, place), axis=0))
        return given

    def body(where_ref, counts_ref, h_ref, *refs):
        g_refs, o_refs = refs[:halves], refs[halves:]
        e = pl.program_id(0)
        row = where_ref[1]
        live = lax.broadcasted_iota(jnp.int32, (tokens, 1), 0) < counts_ref[e]
        h = jnp.where(live, h_ref[0], jnp.zeros((), h_ref.dtype))
        for y in range(halves):
            res = lax.dot_general(
                h, g_refs[y][0], (((0,), (0,)), ((), ())), preferred_element_type=jnp.float32
            )
            res = res.astype(jnp.bfloat16).reshape(rows, chunks, piece, block_d)
            for r in range(rows):
                spot = {"col": 2 * y, "row": r ^ row}
                for j in range(chunks):
                    o_refs[j][flat_index(orders[j], spot), 0] = res[r, j]

    def g_map(y):
        return lambda e, where_ref, counts_ref: (e, 0, ((2 * y) ^ where_ref[2]) + where_ref[0])

    where = jnp.stack([core, place["row"], place["col"] - (place["col"] & 1)]).astype(jnp.int32)
    out = jax.ShapeDtypeStruct((blocks, experts, piece, block_d), jnp.bfloat16)
    return pl.pallas_call(
        body,
        grid_spec=pltpu.PrefetchScalarGridSpec(
            num_scalar_prefetch=2,
            grid=(experts,),
            in_specs=[pl.BlockSpec((1, tokens, features), lambda e, a, b: (e, 0, 0))]
            + [pl.BlockSpec((1, tokens, block_d), g_map(y)) for y in range(halves)],
            out_specs=[
                pl.BlockSpec((blocks, 1, piece, block_d), lambda e, a, b: (0, e, 0, 0))
                for _ in range(chunks)
            ],
        ),
        out_shape=[out] * chunks,
        cost_estimate=pl.CostEstimate(
            flops=experts * tokens * features * outs, bytes_accessed=8000000, transcendentals=0
        ),
    )(where, live_counts, hidden, *([grad_out] * halves))


def copies(token, master, momentum):
    experts, block_f, block_d = master.shape
    step = max(n for n in range(1, 7) if experts % n == 0)

    def body(token_ref, w_ref, m_ref, w_out, m_out):
        w_out[...] = w_ref[...]
        m_out[...] = m_ref[...]

    block = pl.BlockSpec((step, block_f, block_d), lambda i: (i, 0, 0))
    return pl.pallas_call(
        body,
        grid=(experts // step,),
        in_specs=[pl.BlockSpec(memory_space=pl.ANY), block, block],
        out_specs=[block, block],
        out_shape=[
            jax.ShapeDtypeStruct(master.shape, master.dtype),
            jax.ShapeDtypeStruct(momentum.shape, momentum.dtype),
        ],
        cost_estimate=pl.CostEstimate(
            flops=2 * 10**9, bytes_accessed=16 * master.size, transcendentals=0
        ),
    )(token, master, momentum)


def shadow_rows(token, shadow_ids, master, momentum):
    experts = shadow_ids.shape[0]
    block_f, block_d = master.shape[1:]

    def body(ids_ref, token_ref, w_ref, m_ref, w_out, m_out):
        w_out[...] = w_ref[...]
        m_out[...] = m_ref[...]

    row = pl.BlockSpec((1, block_f, block_d), lambda e, ids: (ids[e], 0, 0))
    own = pl.BlockSpec((1, block_f, block_d), lambda e, ids: (e, 0, 0))
    out = jax.ShapeDtypeStruct((experts, block_f, block_d), jnp.float32)
    return pl.pallas_call(
        body,
        grid_spec=pltpu.PrefetchScalarGridSpec(
            num_scalar_prefetch=1,
            grid=(experts,),
            in_specs=[pl.BlockSpec(memory_space=pl.ANY), row, row],
            out_specs=[own, own],
        ),
        out_shape=[out, out],
        cost_estimate=pl.CostEstimate(
            flops=5 * 10**8, bytes_accessed=16 * experts * block_f * block_d, transcendentals=0
        ),
    )(shadow_ids, token, master, momentum)


def place_rows(shadow_ids, new_master, new_momentum, master, momentum):
    experts, block_f, block_d = new_master.shape

    def body(ids_ref, nw_ref, nm_ref, w_ref, m_ref, w_out, m_out):
        w_out[...] = nw_ref[...]
        m_out[...] = nm_ref[...]

    row = pl.BlockSpec((1, block_f, block_d), lambda e, ids: (ids[e], 0, 0))
    own = pl.BlockSpec((1, block_f, block_d), lambda e, ids: (e, 0, 0))
    whole = pl.BlockSpec(memory_space=pl.ANY)
    return pl.pallas_call(
        body,
        grid_spec=pltpu.PrefetchScalarGridSpec(
            num_scalar_prefetch=1,
            grid=(experts,),
            in_specs=[own, own, whole, whole],
            out_specs=[row, row],
        ),
        out_shape=[
            jax.ShapeDtypeStruct(master.shape, master.dtype),
            jax.ShapeDtypeStruct(momentum.shape, momentum.dtype),
        ],
        input_output_aliases={3: 0, 4: 1},
        cost_estimate=pl.CostEstimate(
            flops=5 * 10**8, bytes_accessed=16 * experts * block_f * block_d, transcendentals=0
        ),
    )(shadow_ids, new_master, new_momentum, master, momentum)


def swap(values, name, bit):
    size = lax.axis_size(name)
    return lax.ppermute(values, name, [(i, i ^ (1 << bit)) for i in range(size)])


def add(a, b):
    return (a.astype(jnp.float32) + b.astype(jnp.float32)).astype(jnp.bfloat16)


def shards(hidden, grad_out, counts, shadow_ids, master, momentum):
    rows, cols = lax.axis_size("row"), lax.axis_size("col")
    place = {"row": lax.axis_index("row"), "col": lax.axis_index("col")}
    block_f, block_d = master.shape[1:]
    chunks = chunk_count(block_f)
    live_counts = counts[0]
    core = place["col"] & 1

    col_bits = [("col", k) for k in range(1, bits_of(cols))]
    row_bits = [("row", k) for k in range(bits_of(rows))]
    early = col_bits[:1] + row_bits[:2]
    late = col_bits[1:] + row_bits[2:]
    turns = [j % len(early) for j in range(chunks)]
    orders = [early[t:] + early[:t] + late for t in turns]

    away = half_gradient(hidden, grad_out, live_counts, 1 - core, place, rows, cols, orders)
    got = [swap(a, "col", 0) for a in away]
    own = list(half_gradient(hidden, grad_out, live_counts, core, place, rows, cols, orders))

    for step in range(len(early)):
        sends = []
        for j in range(chunks):
            half = own[j].shape[0] // 2
            sends.append(add(own[j][half:], got[j][half:]))
            own[j], came = add(own[j][:half], got[j][:half]), sends[j]
            got[j] = swap(came, *orders[j][step])
        if step == 0:
            made = copies(sends[-1][0, 0, :8], master, momentum)
            made, own = lax.optimization_barrier((made, own))
        if step == 1:
            old = shadow_rows(sends[-1][0, 0, :8], shadow_ids, master, momentum)
            old, own = lax.optimization_barrier((old, own))
    own = jnp.concatenate(own, axis=2)
    got = jnp.concatenate(got, axis=2)
    for at in late:
        half = own.shape[0] // 2
        send = add(own[half:], got[half:])
        own, got = add(own[:half], got[:half]), swap(send, *at)
    total = own[0].astype(jnp.float32) + got[0].astype(jnp.float32)

    master_copy, momentum_copy = made
    old_master, old_momentum = old
    devices = rows * cols
    scale = jnp.float32((hidden.shape[1] * devices) ** (-0.5))
    new_momentum = momentum_decay * old_momentum + total * scale
    new_master = old_master - step_size * new_momentum
    shadow = new_master.astype(jnp.bfloat16)[None]
    placed = place_rows(
        shadow_ids, new_master, new_momentum, master_copy, momentum_copy
    )
    for bit in range(bits_of(cols) - 1, -1, -1):
        other = swap(shadow, "col", bit)
        if bit == bits_of(cols) - 1:
            placed, shadow = lax.optimization_barrier((placed, shadow))
        shadow = jnp.stack([shadow, other], axis=1).reshape((-1,) + shadow.shape[1:])
    shadow_out = jnp.concatenate(
        [lax.dynamic_index_in_dim(shadow, c ^ place["col"], 0, keepdims=False) for c in range(cols)],
        axis=2,
    )
    return (placed[0], placed[1], shadow_out)


def solution(mesh):
    return jax.shard_map(
        shards,
        mesh=mesh,
        in_specs=(
            P(None, ("row", "col"), None),
            P(None, ("row", "col"), None),
            P(("row", "col"), None),
            P(),
            P(None, "row", "col"),
            P(None, "row", "col"),
        ),
        out_specs=(P(None, "row", "col"), P(None, "row", "col"), P(None, "row", None)),
        check_vma=False,
    )
```
